32 devices in a mesh: dp: 8 (over y, x, core), tensor: 4 (over z).
Axes of the slice: x: 2, y: 2, z: 4, core: 2. Of those that a mesh axis runs over, the one named last changes fastest.
Arguments:
- momentum: float32 [8, 5120, 1024], P('dp', None, 'tensor'), may hold values from -6 to 6
- activations: bfloat16 [4096, 5120], P(('dp', 'tensor')), may hold values from -6 to 6
- out_grads: bfloat16 [4096, 1024], P('dp', 'tensor'), may hold values from -0.29882812 to 0.29882812
- positions: int32 [8, 16, 4, 5120], P('dp', 'tensor'), may hold values from 0 to 63, as said below
Outputs:
- new_momentum: float32 [8, 5120, 1024], P('dp', None, 'tensor')
- update: bfloat16 [5120, 1024], P(None, 'tensor')
The draws below stay inside these ranges and needn't reach their ends.
Inputs may be any that keep to these rules, and one draw needn't show every extreme that they name: The 4 positions of one block of one row of one replica are all different.
All inputs are finite; a program needn't handle non-finite values.
Results may differ from the reference program's by a relative error of at most 0.00075.
Values may be sent and summed in bfloat16 or wider, within the bound.
No kernel may reach another device: no remote copies, remote signals or barrier semaphores. Data moves between devices by JAX's collectives and lax.ppermute only.
A program may use at most 128 MiB of HBM per device.

```python
import jax
import jax.numpy as jnp
from jax import lax

D = 5120
KVW = 1024
SPAN = 64
PICKS = 4
TOK_DEV = 128
TOKENS = 4096
BLOCKS_ROW = 16
N_DP = 8
N_TENSOR = 4


def draw_positions(key, part):
    first_key, second_key = jax.random.split(jax.random.fold_in(key, 17))
    width = SPAN // PICKS
    base = jax.random.randint(first_key, (N_DP, BLOCKS_ROW, 1, D), 0, SPAN)
    offsets = jax.random.randint(second_key, (N_DP, BLOCKS_ROW, PICKS, D), 0, width)
    windows = width * jnp.arange(PICKS, dtype=jnp.int32)[None, None, :, None]
    return ((base + windows + offsets) % SPAN).astype(jnp.int32)


def block_levels(stream_key, extent, pieces, smallest, high):
    level = 1.0
    for position, blocks in pieces:
        draws = jax.random.uniform(jax.random.fold_in(jax.random.fold_in(stream_key, 6), position), (blocks,), jnp.float32, smallest / len(pieces), high / len(pieces))
        level = level * jnp.repeat(jnp.exp(draws), extent[position] // blocks).reshape((-1,) + (1,) * (len(extent) - 1 - position))
    return level


def centred(key, shape, scale, reach, pieces=(), kind=jnp.bfloat16):
    entries = jax.random.normal(key, shape, jnp.float32) * scale
    if len(pieces) > 0:
        entries = block_levels(key, shape, pieces, -0.22, 0.18) * entries
    return jnp.clip(entries, min=-reach, max=reach).astype(kind)


def setup_inputs(seed: int = 0) -> dict:
    key_list = jax.random.split(jax.random.key(seed), 5)
    return {
        "momentum": centred(key_list[0], (N_DP, D, KVW), 1.0, 6.0, ((0, 8), (2, 4)), jnp.float32),
        "activations": centred(key_list[1], (TOKENS, D), 1.0, 6.0, ((0, 32),)),
        "out_grads": centred(key_list[2], (TOKENS, KVW), 0.05, 0.29882812, ((0, 8), (1, 4))),
        "positions": draw_positions(jax.random.fold_in(key_list[4], 71), 0),
    }


def dct_table():
    freq = jnp.arange(64, dtype=jnp.float32)[:, None]
    place = jnp.arange(64, dtype=jnp.float32)[None, :]
    scales = jnp.where(freq == 0, jnp.float32(1.0 / 8.0), jnp.float32((2.0 / 64.0) ** 0.5))
    return scales * jnp.cos(jnp.float32(jnp.pi) * (2.0 * place + 1.0) * freq / 128.0)

def reference(momentum, activations, out_grads, positions):
    cosines = dct_table()
    inputs_rep = activations.reshape(N_DP, TOK_DEV * N_TENSOR, D)
    grads_rep = out_grads.reshape(N_DP, TOK_DEV * N_TENSOR, KVW)
    lane_ids = jnp.arange(64, dtype=jnp.int32)

    def per_replica(summed, record):
        moment_one, inputs_one, grads_one, picks_one = record
        gradient = jnp.dot(inputs_one.T, grads_one, preferred_element_type=jnp.float32)
        accumulated = 0.9 * moment_one + gradient
        coeffs = jnp.dot(accumulated.reshape(-1, 64), cosines.T, precision=lax.Precision.HIGHEST)
        coeffs = coeffs.reshape(D, KVW // 64, 64)
        hits = jnp.where(picks_one[:, :, None, :] == lane_ids[None, None, :, None], 1.0, 0.0)
        chosen = lax.optimization_barrier(jnp.sum(hits, axis=1)).transpose(2, 0, 1).astype(coeffs.dtype)
        own_tile = coeffs * chosen
        restored = jnp.dot(own_tile.reshape(-1, 64), cosines, precision=lax.Precision.HIGHEST)
        return (summed + own_tile, accumulated - restored.reshape(D, KVW))
    start_sum = jnp.zeros((D, KVW // 64, 64), jnp.float32)
    summed, new_momentum = lax.scan(per_replica, start_sum, (momentum, inputs_rep, grads_rep, positions))
    decoded = jnp.dot(summed.reshape(-1, 64), cosines, precision=lax.Precision.HIGHEST).reshape(D, KVW)
    row_scale = jnp.sqrt(lax.optimization_barrier(jnp.mean(decoded * decoded, axis=1, keepdims=True)) + 1e-05)
    update = (decoded / row_scale).astype(jnp.bfloat16)
    return (new_momentum, update)
```

```python
import functools

import jax
import jax.numpy as jnp
import numpy as np
from jax import lax
from jax.experimental import pallas as pl
from jax.experimental.pallas import tpu as pltpu
from jax.sharding import PartitionSpec as P


SPAN = 64
SUB = 256
LANES = 128
CODE_TOP = 32764.0
LN2 = 0.6931471805599453
VMEM_LIMIT = 40 * 1024 * 1024
CHUNKS = (6, 6, 4, 4)
GROUPS = ((0, 1), (2, 3))


def basis_parts(spans):
    freq = np.arange(SPAN, dtype=np.float64)[:, None]
    place = np.arange(SPAN, dtype=np.float64)[None, :]
    scales = np.where(freq == 0, (1.0 / SPAN) ** 0.5, (2.0 / SPAN) ** 0.5)
    table = scales * np.cos(np.pi * (2.0 * place + 1.0) * freq / (2 * SPAN))
    whole = np.kron(np.eye(spans), table).astype(np.float32)
    high = whole.astype(jnp.bfloat16)
    low = (whole - high.astype(np.float32)).astype(jnp.bfloat16)
    return np.stack([high, low, high.T, low.T])


def dot32(a, b):
    return lax.dot_general(a, b, (((1,), (0,)), ((), ())), preferred_element_type=jnp.float32)


def dot_split(high, low, x):
    x_high = x.astype(jnp.bfloat16)
    x_low = (x - x_high.astype(jnp.float32)).astype(jnp.bfloat16)
    return dot32(high, x_high) + (dot32(high, x_low) + dot32(low, x_high))


def lanes_at(i, offset=0):
    return pl.ds(pl.multiple_of(offset + i * SUB, SUB), SUB)


def line_blocks(grads_ref, tokens, roles):
    index = lax.axis_index("tensor")
    middle = (index == 1) | (index == 2)
    sources = (index, 3 * (index - 1), 3 - index, 6 - 3 * index)
    parts = []
    for k in roles:
        at = pl.multiple_of(jnp.clip(sources[k], 0, 3) * tokens, tokens)
        part = grads_ref[pl.ds(at, tokens)].T
        parts.append(part if k == 0 else jnp.where(middle, part, jnp.zeros_like(part)))
    return jnp.concatenate(parts, axis=1)


def pairs_of(count, work):
    if count % 2 == 0:
        lax.fori_loop(0, count // 2, lambda i, c: work((2 * i, 2 * i + 1)), None)
    else:
        lax.fori_loop(0, count, lambda i, c: work((i,)), None)


def partial_kernel(count, start, grads_ref, *refs):
    act_refs, out_ref = refs[:3], refs[3]
    act_buf, out_buf, blocks_ref, in_sem, out_sem = refs[4:]
    cols, tokens = grads_ref.shape[1], act_refs[0].shape[0]

    def copy_in(k, i):
        offset = start if k == 0 else 0
        return pltpu.make_async_copy(
            act_refs[k].at[:, lanes_at(i, offset)],
            act_buf.at[pl.ds(k * tokens, tokens), lanes_at(i)],
            in_sem.at[k, i],
        )

    def copy_out(i):
        return pltpu.make_async_copy(
            out_buf.at[:, lanes_at(i)], out_ref.at[:, lanes_at(i)], out_sem.at[i]
        )

    for i in range(count):
        for k in range(len(act_refs)):
            copy_in(k, i).start()

    blocks_ref[...] = line_blocks(grads_ref, tokens, (0, 2, 3))

    def one(i):
        for k in range(len(act_refs)):
            copy_in(k, i).wait()
        part = dot32(blocks_ref[...], act_buf[:, lanes_at(i)])
        top = jnp.maximum(jnp.max(jnp.abs(part), axis=0, keepdims=True), 1e-30)
        level = jnp.floor(jnp.log(top) * (1.0 / LN2)) + 1.0
        code = jnp.round(part * (CODE_TOP * jnp.exp(-level * LN2)))
        out_buf[:cols, lanes_at(i)] = code.astype(jnp.int32).astype(jnp.int16)
        extra = jnp.broadcast_to(level.astype(jnp.int32), (out_buf.shape[0] - cols, SUB))
        out_buf[cols:, lanes_at(i)] = extra.astype(jnp.int16)
        copy_out(i).start()

    def work(tiles):
        for i in tiles:
            one(i)

    pairs_of(count, work)
    for i in range(count):
        copy_out(i).wait()


def grad_kernel(n_act, has_part, slots, count, start, base, *refs):
    basis_ref, grads_ref, moment_ref, picks_ref = refs[:4]
    act_refs = refs[4 : 4 + n_act]
    part_ref = refs[4 + n_act] if has_part else None
    new_ref, record_ref = refs[-15:-13]
    moment_buf, picks_buf, act_buf, part_buf, new_buf, record_buf = refs[-13:-7]
    coeffs_refs, tile_refs, blocks_ref, in_sem, out_sem = refs[-7:-5], refs[-5:-3], *refs[-3:]
    cols = moment_ref.shape[2]
    spans = cols // SPAN
    tokens = act_refs[0].shape[0]
    ids = lax.broadcasted_iota(jnp.int32, (SPAN, LANES), 0)

    def copies_in(i):
        pairs = [
            (moment_ref.at[0, lanes_at(i, start)], moment_buf.at[i]),
            (picks_ref.at[0, :, :, lanes_at(i, start)], picks_buf.at[i]),
        ]
        for k, ref in enumerate(act_refs):
            offset = start if k == 0 else 0
            pairs.append(
                (ref.at[:, lanes_at(i, offset)], act_buf.at[i, pl.ds(k * tokens, tokens)])
            )
        if has_part:
            pairs.append((part_ref.at[:, lanes_at(i)], part_buf.at[i]))
        return [pltpu.make_async_copy(a, b, in_sem.at[k, i]) for k, (a, b) in enumerate(pairs)]

    def copies_out(i):
        return [
            pltpu.make_async_copy(
                new_buf.at[i], new_ref.at[0, lanes_at(i, start)], out_sem.at[0, i]
            ),
            pltpu.make_async_copy(
                record_buf.at[i], record_ref.at[:, lanes_at(i, start - base)], out_sem.at[1, i]
            ),
        ]

    for i in range(count):
        for copy in copies_in(i):
            copy.start()

    if n_act > 1:
        blocks_ref[...] = line_blocks(grads_ref, tokens, (0, 1, 2, 3))
    else:
        blocks_ref[...] = grads_ref[...].T

    def gather(i, coeffs_ref):
        for copy in copies_in(i):
            copy.wait()
        total = 0.9 * moment_buf[i].T + dot32(blocks_ref[...], act_buf[i])
        if has_part:
            level = part_buf[i, cols:][:1].astype(jnp.int32).astype(jnp.float32)
            code = part_buf[i, :cols].astype(jnp.int32).astype(jnp.float32)
            total = total + code * (jnp.exp(level * LN2) * (1.0 / CODE_TOP))
        coeffs_ref[...] = dot_split(basis_ref[0], basis_ref[1], total)
        return total

    def pick(i, coeffs_ref, tile_ref):
        for lo in range(0, SUB, LANES):
            lanes = slice(lo, lo + LANES)
            for b in range(spans):
                block = coeffs_ref[b * SPAN : (b + 1) * SPAN, lanes]
                tile = jnp.zeros_like(block)
                code = jnp.zeros((1, LANES), jnp.int32)
                for j in range(slots):
                    place = picks_buf[i, b, j : j + 1, lanes]
                    hit = place == ids
                    value = jnp.sum(jnp.where(hit, block, 0.0), axis=0, keepdims=True)
                    tile = jnp.where(hit, block, tile)
                    record_buf[i, b * slots + j : b * slots + j + 1, lanes] = value
                    code = code + place * SPAN**j
                tile_ref[b * SPAN : (b + 1) * SPAN, lanes] = tile
                row = spans * slots + b
                record_buf[i, row : row + 1, lanes] = code.astype(jnp.float32)

    def finish(i, total, tile_ref):
        restored = dot_split(basis_ref[2], basis_ref[3], tile_ref[...])
        new_buf[i] = (total - restored).T
        for copy in copies_out(i):
            copy.start()

    def work(tiles):
        totals = [gather(i, coeffs_refs[k]) for k, i in enumerate(tiles)]
        for k, i in enumerate(tiles):
            pick(i, coeffs_refs[k], tile_refs[k])
            finish(i, totals[k], tile_refs[k])

    pairs_of(count, work)
    for i in range(count):
        for copy in copies_out(i):
            copy.wait()


def sum_kernel(n_rec, slots, count, *refs):
    basis_ref = refs[0]
    record_refs = refs[1 : 1 + n_rec]
    decoded_ref, squares_ref, record_buf, decoded_buf = refs[1 + n_rec : 5 + n_rec]
    place_ref, tile_refs, in_sem, out_sem = refs[5 + n_rec], refs[6 + n_rec : 8 + n_rec], *refs[8 + n_rec :]
    cols = decoded_ref.shape[0]
    spans = cols // SPAN
    ids = lax.broadcasted_iota(jnp.int32, (SPAN, LANES), 0)

    def copy_in(k, i):
        return pltpu.make_async_copy(
            record_refs[k].at[:, lanes_at(i)], record_buf.at[k, i], in_sem.at[k, i]
        )

    def copy_out(i):
        return pltpu.make_async_copy(
            decoded_buf.at[i], decoded_ref.at[:, lanes_at(i)], out_sem.at[i]
        )

    for i in range(count):
        for k in range(n_rec):
            copy_in(k, i).start()

    def spread(slot, i):
        for k in range(n_rec):
            copy_in(k, i).wait()
            code = record_buf[k, i, spans * slots :].astype(jnp.int32)
            for j in range(slots):
                place_ref[slot, k, j] = lax.shift_right_logical(code, 6 * j) & (SPAN - 1)
        for lo in range(0, SUB, LANES):
            lanes = slice(lo, lo + LANES)
            for b in range(spans):
                stack = []
                for k in range(n_rec):
                    tile = jnp.zeros((SPAN, LANES), jnp.float32)
                    for j in range(slots):
                        place = place_ref[slot, k, j, b : b + 1, lanes]
                        value = record_buf[k, i, b * slots + j : b * slots + j + 1, lanes]
                        tile = jnp.where(place == ids, value, tile)
                    stack.append(tile)
                    done = k + 1
                    while done % 2 == 0:
                        right = stack.pop()
                        stack[-1] = stack[-1] + right
                        done //= 2
                tile_refs[slot][b * SPAN : (b + 1) * SPAN, lanes] = stack[0]

    def decode(slot, i):
        decoded = dot_split(basis_ref[2], basis_ref[3], tile_refs[slot][...])
        decoded_buf[i] = decoded
        squares_ref[:, lanes_at(i)] = jnp.sum(decoded * decoded, axis=0, keepdims=True)
        copy_out(i).start()

    def work(tiles):
        for slot, i in enumerate(tiles):
            spread(slot, i)
            decode(slot, i)

    pairs_of(count, work)
    for i in range(count):
        copy_out(i).wait()


def scale_kernel(n_sq, n_all, count, start, *refs):
    decoded_ref, sq_refs = refs[0], refs[1 : 1 + n_sq]
    out_ref, decoded_buf, out_buf, in_sem, out_sem = refs[-5:]

    def copy_in(i):
        return pltpu.make_async_copy(
            decoded_ref.at[:, lanes_at(i)], decoded_buf.at[i], in_sem.at[i]
        )

    def copy_out(i):
        return pltpu.make_async_copy(
            out_buf.at[i], out_ref.at[lanes_at(i, start)], out_sem.at[i]
        )

    for i in range(count):
        copy_in(i).start()

    def step(i, carry):
        total = sq_refs[0][:, lanes_at(i)]
        for ref in sq_refs[1:]:
            total = total + ref[:, lanes_at(i)]
        scale = 1.0 / jnp.sqrt(total * (1.0 / n_all) + 1e-05)
        copy_in(i).wait()
        out_buf[i] = (decoded_buf[i] * scale).astype(jnp.bfloat16).T
        copy_out(i).start()
        return carry

    lax.fori_loop(0, count, step, 0)
    for i in range(count):
        copy_out(i).wait()


def call(kernel, out_shape, n_vmem, scratch, aliases, flops, moved, args):
    vmem = pl.BlockSpec(memory_space=pltpu.VMEM)
    anywhere = pl.BlockSpec(memory_space=pl.ANY)
    many = [anywhere if where == "hbm" else vmem for _, where in out_shape]
    return pl.pallas_call(
        kernel,
        in_specs=[vmem if k in n_vmem else anywhere for k in range(len(args))],
        out_specs=many,
        out_shape=[shape for shape, _ in out_shape],
        scratch_shapes=scratch,
        input_output_aliases=aliases,
        compiler_params=pltpu.CompilerParams(vmem_limit_bytes=VMEM_LIMIT),
        cost_estimate=pl.CostEstimate(flops=flops, bytes_accessed=moved, transcendentals=0),
    )(*args)


def body(momentum, activations, out_grads, positions):
    rows, cols = momentum.shape[1:]
    spans, slots = positions.shape[1:3]
    tokens = activations.shape[0]
    n_tensor, n_dp = lax.axis_size("tensor"), lax.axis_size("dp")
    n_tiles = rows // SUB
    edges = [0]
    for c in CHUNKS:
        edges.append(edges[-1] + c)
    edges = [e * n_tiles // edges[-1] for e in edges]
    basis = jnp.asarray(basis_parts(spans))
    n_rows = spans * slots + spans
    dma = pltpu.SemaphoreType.DMA
    f32, bf16 = jnp.float32, jnp.bfloat16

    line = n_tensor == 4
    if line:
        outer, back = [(0, 1), (3, 2)], [(1, 0), (2, 3)]
        inner = []
        for d in range(n_dp):
            for t, to in ((0, (d ^ 1, 0)), (1, (d, 2)), (2, (d, 1)), (3, (d ^ 1, 3))):
                inner.append((d * n_tensor + t, to[0] * n_tensor + to[1]))
        other_grads = lax.ppermute(out_grads, "tensor", outer)
        owns = []
        for c in range(len(CHUNKS)):
            owns.append(lax.slice_in_dim(activations, edges[c] * SUB, edges[c + 1] * SUB, axis=1))
    else:
        gathered = lax.all_gather(activations, "tensor", axis=0, tiled=True)

    def add_chunk(c, base, group_width, new_momentum, record):
        start, count = edges[c] * SUB, edges[c + 1] - edges[c]
        width = count * SUB
        args = [basis, out_grads, momentum, positions]
        n_act = 4 if line else 1
        if line:
            own = owns[c]
            one = lax.ppermute(own, "tensor", outer)
            two = lax.ppermute(own, ("dp", "tensor"), inner)
            three = lax.ppermute(one, ("dp", "tensor"), inner)
            (coded,) = call(
                functools.partial(partial_kernel, count, start),
                [(jax.ShapeDtypeStruct((cols + 16, width), jnp.int16), "hbm")],
                (0,),
                [
                    pltpu.VMEM((3 * tokens, width), bf16),
                    pltpu.VMEM((cols + 16, width), jnp.int16),
                    pltpu.VMEM((cols, 3 * tokens), bf16),
                    dma((3, count)),
                    dma((count,)),
                ],
                {},
                2 * cols * 3 * tokens * width,
                2 * width * (3 * tokens + cols),
                [other_grads, activations, two, three],
            )
            part = lax.ppermute(coded, "tensor", back)
            args += [activations, one, two, three, part]
        else:
            args += [gathered]
        aliases = {}
        for place, buffer in enumerate((new_momentum, record)):
            if buffer is not None:
                aliases[len(args)] = place
                args.append(buffer)
        return call(
            functools.partial(grad_kernel, n_act, line, slots, count, start, base),
            [
                (jax.ShapeDtypeStruct(momentum.shape, f32), "hbm"),
                (jax.ShapeDtypeStruct((n_rows, group_width), f32), "hbm"),
            ],
            (0, 1),
            [
                pltpu.VMEM((count, SUB, cols), f32),
                pltpu.VMEM((count, spans, slots, SUB), jnp.int32),
                pltpu.VMEM((count, n_tensor * tokens, SUB), bf16),
                pltpu.VMEM((count, cols + 16, SUB), jnp.int16),
                pltpu.VMEM((count, SUB, cols), f32),
                pltpu.VMEM((count, n_rows, SUB), f32),
                pltpu.VMEM((cols, SUB), f32),
                pltpu.VMEM((cols, SUB), f32),
                pltpu.VMEM((cols, SUB), f32),
                pltpu.VMEM((cols, SUB), f32),
                pltpu.VMEM((cols, n_tensor * tokens), bf16),
                dma((n_act + 3, count)),
                dma((2, count)),
            ],
            aliases,
            2 * cols * n_tensor * tokens * width + 12 * cols * cols * width,
            width * (8 * cols + 10 * tokens),
            args,
        )

    new_momentum, update = None, None
    for group in GROUPS:
        base, count = edges[group[0]] * SUB, edges[group[-1] + 1] - edges[group[0]]
        width = count * SUB
        record = None
        for c in group:
            new_momentum, record = add_chunk(c, base, width, new_momentum, record)
        near = [record]
        for k in range(1, n_dp // 2):
            near.append(lax.ppermute(record, "dp", [(i, i ^ (2 * k)) for i in range(n_dp)]))
        records = []
        for r in near:
            records += [r, lax.ppermute(r, "dp", [(i, i ^ 1) for i in range(n_dp)])]
        decoded, squares = call(
            functools.partial(sum_kernel, n_dp, slots, count),
            [
                (jax.ShapeDtypeStruct((cols, width), f32), "hbm"),
                (jax.ShapeDtypeStruct((1, width), f32), "vmem"),
            ],
            (0,),
            [
                pltpu.VMEM((n_dp, count, n_rows, SUB), f32),
                pltpu.VMEM((count, cols, SUB), f32),
                pltpu.VMEM((2, n_dp, slots, spans, SUB), jnp.int32),
                pltpu.VMEM((cols, SUB), f32),
                pltpu.VMEM((cols, SUB), f32),
                dma((n_dp, count)),
                dma((count,)),
            ],
            {},
            6 * cols * cols * width,
            width * 4 * (cols + n_dp * n_rows),
            [basis] + records,
        )
        if line:
            sq_args = [squares]
            for k in range(n_tensor - 1, 0, -1):
                pairs = [(i, i ^ k) for i in range(n_tensor)]
                sq_args.append(lax.ppermute(squares, "tensor", pairs))
        else:
            sq_args = [lax.psum(squares, "tensor")]
        args = [decoded] + sq_args
        aliases = {}
        if update is not None:
            aliases = {len(args): 0}
            args.append(update)
        (update,) = call(
            functools.partial(scale_kernel, len(sq_args), cols * n_tensor, count, base),
            [(jax.ShapeDtypeStruct((rows, cols), bf16), "hbm")],
            range(1, 1 + len(sq_args)),
            [
                pltpu.VMEM((count, cols, SUB), f32),
                pltpu.VMEM((count, SUB, cols), bf16),
                dma((count,)),
                dma((count,)),
            ],
            aliases,
            width * cols,
            width * cols * 6,
            args,
        )
    return new_momentum, update


def solution(mesh):
    placed = (
        P("dp", None, "tensor"),
        P(("dp", "tensor"), None),
        P("dp", "tensor"),
        P("dp", "tensor", None, None),
    )
    return jax.shard_map(
        body,
        mesh=mesh,
        in_specs=placed,
        out_specs=(P("dp", None, "tensor"), P(None, "tensor")),
        check_vma=False,
    )
```

```python
import functools

import jax
import jax.numpy as jnp
import numpy as np
from jax import lax
from jax.experimental import pallas as pl
from jax.experimental.pallas import tpu as pltpu
from jax.sharding import PartitionSpec as P


SPAN = 64
SUB = 256
LANES = 128
SUBLANES = 8
CODE_TOP = 32764.0
LN2 = 0.6931471805599453
VMEM_LIMIT = 40 * 1024 * 1024
CHUNKS = (4, 4, 6, 6)
GROUPS = ((0, 1), (2,), (3,))


def basis_parts():
    freq = np.arange(SPAN, dtype=np.float64)[:, None]
    place = np.arange(SPAN, dtype=np.float64)[None, :]
    scales = np.where(freq == 0, (1.0 / SPAN) ** 0.5, (2.0 / SPAN) ** 0.5)
    table = scales * np.cos(np.pi * (2.0 * place + 1.0) * freq / (2 * SPAN))
    table = table.astype(np.float32)
    high = table.astype(jnp.bfloat16)
    low = (table - high.astype(np.float32)).astype(jnp.bfloat16)
    return np.stack([np.concatenate(p, axis=1) for p in ((high, high, low), (high.T, high.T, low.T))])


def dot32(a, b):
    return lax.dot_general(a, b, (((1,), (0,)), ((), ())), preferred_element_type=jnp.float32)


def dot_split(triple, x):
    high = x.astype(jnp.bfloat16)
    low = (x - high.astype(jnp.float32)).astype(jnp.bfloat16)
    outs = []
    for at in range(0, x.shape[0], SPAN):
        part = high[at : at + SPAN]
        outs.append(dot32(triple, jnp.concatenate([part, low[at : at + SPAN], part], axis=0)))
    return jnp.concatenate(outs, axis=0)


def lanes_at(i, offset=0):
    return pl.ds(pl.multiple_of(offset + i * SUB, SUB), SUB)


def line_blocks(grads_ref, tokens, roles):
    index = lax.axis_index("tensor")
    middle = (index == 1) | (index == 2)
    sources = (index, 3 * (index - 1), 3 - index, 6 - 3 * index)
    parts = []
    for k in roles:
        at = pl.multiple_of(jnp.clip(sources[k], 0, 3) * tokens, tokens)
        part = grads_ref[pl.ds(at, tokens)].T
        parts.append(part if k == 0 else jnp.where(middle, part, jnp.zeros_like(part)))
    return jnp.concatenate(parts, axis=1)


def pairs_of(count, work):
    lax.fori_loop(0, count // 2, lambda i, c: work((2 * i, 2 * i + 1)), None)
    if count % 2:
        work((count - 1,))


def partial_kernel(count, start, grads_ref, *refs):
    act_refs, out_ref = refs[:3], refs[3]
    act_buf, out_buf, blocks_ref, in_sem, out_sem = refs[4:]
    cols, tokens = grads_ref.shape[1], act_refs[0].shape[0]

    def copy_in(k, i):
        offset = start if k == 0 else 0
        return pltpu.make_async_copy(
            act_refs[k].at[:, lanes_at(i, offset)],
            act_buf.at[pl.ds(k * tokens, tokens), lanes_at(i)],
            in_sem.at[k, i],
        )

    def copy_out(i):
        return pltpu.make_async_copy(
            out_buf.at[:, lanes_at(i)], out_ref.at[:, lanes_at(i)], out_sem.at[i]
        )

    for i in range(count):
        for k in range(len(act_refs)):
            copy_in(k, i).start()

    blocks_ref[...] = line_blocks(grads_ref, tokens, (0, 2, 3))

    def one(i):
        for k in range(len(act_refs)):
            copy_in(k, i).wait()
        part = dot32(blocks_ref[...], act_buf[:, lanes_at(i)])
        top = jnp.maximum(jnp.max(jnp.abs(part), axis=0, keepdims=True), 1e-30)
        level = jnp.floor(jnp.log(top) * (1.0 / LN2)) + 1.0
        code = jnp.round(part * (CODE_TOP * jnp.exp(-level * LN2)))
        out_buf[:cols, lanes_at(i)] = code.astype(jnp.int32).astype(jnp.int16)
        extra = jnp.broadcast_to(level.astype(jnp.int32), (out_buf.shape[0] - cols, SUB))
        out_buf[cols:, lanes_at(i)] = extra.astype(jnp.int16)
        copy_out(i).start()

    def work(tiles):
        for i in tiles:
            one(i)

    pairs_of(count, work)
    for i in range(count):
        copy_out(i).wait()


def grad_kernel(n_act, has_part, slots, count, start, base, *refs):
    basis_ref, grads_ref, moment_ref, picks_ref = refs[:4]
    act_refs = refs[4 : 4 + n_act]
    part_ref = refs[4 + n_act] if has_part else None
    new_ref, record_ref = refs[-15:-13]
    moment_buf, picks_buf, act_buf, part_buf, new_buf, record_buf = refs[-13:-7]
    coeffs_refs, tile_refs, blocks_ref, in_sem, out_sem = refs[-7:-5], refs[-5:-3], *refs[-3:]
    cols = moment_ref.shape[2]
    spans = cols // SPAN
    tokens = act_refs[0].shape[0]
    ids = lax.broadcasted_iota(jnp.int32, (SUBLANES, LANES), 0)

    def copies_in(i):
        pairs = [
            (moment_ref.at[0, lanes_at(i, start)], moment_buf.at[i]),
            (picks_ref.at[0, :, :, lanes_at(i, start)], picks_buf.at[i]),
        ]
        for k, ref in enumerate(act_refs):
            offset = start if k == 0 else 0
            pairs.append(
                (ref.at[:, lanes_at(i, offset)], act_buf.at[i, pl.ds(k * tokens, tokens)])
            )
        if has_part:
            pairs.append((part_ref.at[:, lanes_at(i)], part_buf.at[i]))
        return [pltpu.make_async_copy(a, b, in_sem.at[k, i]) for k, (a, b) in enumerate(pairs)]

    def copies_out(i):
        return [
            pltpu.make_async_copy(
                new_buf.at[i], new_ref.at[0, lanes_at(i, start)], out_sem.at[0, i]
            ),
            pltpu.make_async_copy(
                record_buf.at[i], record_ref.at[:, lanes_at(i, start - base)], out_sem.at[1, i]
            ),
        ]

    for i in range(count):
        for copy in copies_in(i):
            copy.start()

    if n_act > 1:
        blocks_ref[...] = line_blocks(grads_ref, tokens, (0, 1, 2, 3))
    else:
        blocks_ref[...] = grads_ref[...].T

    def gather(i, coeffs_ref):
        for copy in copies_in(i):
            copy.wait()
        total = 0.9 * moment_buf[i].T + dot32(blocks_ref[...], act_buf[i])
        if has_part:
            level = part_buf[i, cols:][:1].astype(jnp.int32).astype(jnp.float32)
            code = part_buf[i, :cols].astype(jnp.int32).astype(jnp.float32)
            total = total + code * (jnp.exp(level * LN2) * (1.0 / CODE_TOP))
        coeffs_ref[...] = dot_split(basis_ref[0], total)
        return total

    def pick(i, coeffs_ref, tile_ref):
        for lo in range(0, SUB, LANES):
            lanes = slice(lo, lo + LANES)
            for b in range(spans):
                rows = [b * SPAN + h * SUBLANES for h in range(SPAN // SUBLANES)]
                blocks = [coeffs_ref[at : at + SUBLANES, lanes] for at in rows]
                parts = [jnp.zeros((SUBLANES, LANES), jnp.float32)] * len(rows)
                code = jnp.zeros((1, LANES), jnp.int32)
                for j in range(slots):
                    place = picks_buf[i, b, j : j + 1, lanes]
                    offset = place - ids
                    value = jnp.zeros((SUBLANES, LANES), jnp.float32)
                    for h in range(len(rows)):
                        hit = offset == h * SUBLANES
                        value = jnp.where(hit, blocks[h], value)
                        parts[h] = jnp.where(hit, blocks[h], parts[h])
                    value = jnp.sum(value, axis=0, keepdims=True)
                    record_buf[i, b * slots + j : b * slots + j + 1, lanes] = value
                    code = code + place * SPAN**j
                for at, part in zip(rows, parts):
                    tile_ref[at : at + SUBLANES, lanes] = part
                row = spans * slots + b
                record_buf[i, row : row + 1, lanes] = code.astype(jnp.float32)

    def finish(i, total, tile_ref):
        restored = dot_split(basis_ref[1], tile_ref[...])
        new_buf[i] = (total - restored).T
        for copy in copies_out(i):
            copy.start()

    def work(tiles):
        totals = [gather(i, coeffs_refs[k]) for k, i in enumerate(tiles)]
        for k, i in enumerate(tiles):
            pick(i, coeffs_refs[k], tile_refs[k])
            finish(i, totals[k], tile_refs[k])

    pairs_of(count, work)
    for i in range(count):
        for copy in copies_out(i):
            copy.wait()


def tile_of(i, split, ahead=0):
    return i * split + (lax.axis_index("dp") + ahead) % split


def sum_kernel(n_rec, slots, count, base, split, *refs):
    basis_ref = refs[0]
    record_refs = refs[1 : 1 + n_rec]
    decoded_ref, squares_ref, record_buf, decoded_buf, place_ref = refs[-9:-4]
    tile_refs, in_sem, out_sem = refs[-4:-2], *refs[-2:]
    cols = decoded_ref.shape[0]
    spans = cols // SPAN
    ids = lax.broadcasted_iota(jnp.int32, (SUBLANES, LANES), 0)

    def copy_in(k, i):
        return pltpu.make_async_copy(
            record_refs[k].at[:, lanes_at(tile_of(i, split))], record_buf.at[k, i], in_sem.at[k, i]
        )

    def copy_out(i):
        return pltpu.make_async_copy(
            decoded_buf.at[i], decoded_ref.at[:, lanes_at(i, base)], out_sem.at[i]
        )

    for i in range(count):
        for k in range(n_rec):
            copy_in(k, i).start()

    def spread(slot, i):
        for k in range(n_rec):
            copy_in(k, i).wait()
            code = record_buf[k, i, spans * slots :].astype(jnp.int32)
            for j in range(slots):
                place_ref[slot, k, j] = lax.shift_right_logical(code, 6 * j) & (SPAN - 1)
        for lo in range(0, SUB, LANES):
            lanes = slice(lo, lo + LANES)
            for b in range(spans):
                stack = []
                for k in range(n_rec):
                    parts = [jnp.zeros((SUBLANES, LANES), jnp.float32)] * (SPAN // SUBLANES)
                    for j in range(slots):
                        place = place_ref[slot, k, j, b : b + 1, lanes] - ids
                        value = record_buf[k, i, b * slots + j : b * slots + j + 1, lanes]
                        value = jnp.broadcast_to(value, (SUBLANES, LANES))
                        for h in range(SPAN // SUBLANES):
                            parts[h] = jnp.where(place == h * SUBLANES, value, parts[h])
                    stack.append(parts)
                    done = k + 1
                    while done % 2 == 0:
                        right = stack.pop()
                        stack[-1] = [x + y for x, y in zip(stack[-1], right)]
                        done //= 2
                for h, part in enumerate(stack[0]):
                    at = b * SPAN + h * SUBLANES
                    tile_refs[slot][at : at + SUBLANES, lanes] = part

    def decode(slot, i):
        decoded = dot_split(basis_ref[1], tile_refs[slot][...])
        decoded_buf[i] = decoded
        squares_ref[:, lanes_at(i)] = jnp.sum(decoded * decoded, axis=0, keepdims=True)
        copy_out(i).start()

    def work(tiles):
        for slot, i in enumerate(tiles):
            spread(slot, i)
            decode(slot, i)

    pairs_of(count, work)
    for i in range(count):
        copy_out(i).wait()


def scale_kernel(n_sq, n_all, count, split, *refs):
    decoded_ref, sq_refs = refs[0], refs[1 : 1 + n_sq]
    out_ref, half_ref, decoded_buf, in_sem, out_sem = refs[-5:]

    def copy_in(i):
        return pltpu.make_async_copy(
            decoded_ref.at[:, lanes_at(i)], decoded_buf.at[i], in_sem.at[i]
        )

    def copy_out(i):
        return pltpu.make_async_copy(
            half_ref.at[i], out_ref.at[lanes_at(tile_of(i, split))], out_sem.at[i]
        )

    for i in range(count):
        copy_in(i).start()

    def step(i, carry):
        total = sq_refs[0][:, lanes_at(i)]
        for ref in sq_refs[1:]:
            total = total + ref[:, lanes_at(i)]
        scale = 1.0 / jnp.sqrt(total * (1.0 / n_all) + 1e-05)
        copy_in(i).wait()
        half_ref[i] = (decoded_buf[i] * scale).astype(jnp.bfloat16).T
        copy_out(i).start()
        return carry

    lax.fori_loop(0, count, step, 0)
    for i in range(count):
        copy_out(i).wait()


def place_kernel(count, split, half_ref, update_ref, out_ref, out_sem):
    def copy_out(i):
        return pltpu.make_async_copy(
            half_ref.at[i], out_ref.at[lanes_at(tile_of(i, split, 1))], out_sem.at[i]
        )

    for i in range(count):
        copy_out(i).start()
    for i in range(count):
        copy_out(i).wait()


def call(kernel, out_shape, n_vmem, scratch, aliases, flops, moved, args):
    vmem = pl.BlockSpec(memory_space=pltpu.VMEM)
    anywhere = pl.BlockSpec(memory_space=pl.ANY)
    many = [anywhere if where == "hbm" else vmem for _, where in out_shape]
    return pl.pallas_call(
        kernel,
        in_specs=[vmem if k in n_vmem else anywhere for k in range(len(args))],
        out_specs=many,
        out_shape=[shape for shape, _ in out_shape],
        scratch_shapes=scratch,
        input_output_aliases=aliases,
        compiler_params=pltpu.CompilerParams(vmem_limit_bytes=VMEM_LIMIT),
        cost_estimate=pl.CostEstimate(flops=flops, bytes_accessed=moved, transcendentals=0),
    )(*args)


def body(momentum, activations, out_grads, positions):
    rows, cols = momentum.shape[1:]
    spans, slots = positions.shape[1:3]
    tokens = activations.shape[0]
    n_tensor, n_dp = lax.axis_size("tensor"), lax.axis_size("dp")
    n_tiles = rows // SUB
    edges = [0]
    for c in CHUNKS:
        edges.append(edges[-1] + c)
    edges = [e * n_tiles // edges[-1] for e in edges]
    basis = jnp.asarray(basis_parts())
    n_rows = spans * slots + spans
    dma = pltpu.SemaphoreType.DMA
    f32, bf16 = jnp.float32, jnp.bfloat16

    line = n_tensor == 4
    if line:
        outer, back = [(0, 1), (3, 2)], [(1, 0), (2, 3)]
        inner = []
        for d in range(n_dp):
            for t, to in ((0, (d ^ 1, 0)), (1, (d, 2)), (2, (d, 1)), (3, (d ^ 1, 3))):
                inner.append((d * n_tensor + t, to[0] * n_tensor + to[1]))
        other_grads = lax.ppermute(out_grads, "tensor", outer)
        owns = []
        for c in range(len(CHUNKS)):
            owns.append(lax.slice_in_dim(activations, edges[c] * SUB, edges[c + 1] * SUB, axis=1))
    else:
        gathered = lax.all_gather(activations, "tensor", axis=0, tiled=True)

    def add_chunk(c, base, group_width, new_momentum, record):
        start, count = edges[c] * SUB, edges[c + 1] - edges[c]
        width = count * SUB
        args = [basis, out_grads, momentum, positions]
        n_act = 4 if line else 1
        if line:
            own = owns[c]
            one = lax.ppermute(own, "tensor", outer)
            two = lax.ppermute(own, ("dp", "tensor"), inner)
            three = lax.ppermute(one, ("dp", "tensor"), inner)
            (coded,) = call(
                functools.partial(partial_kernel, count, start),
                [(jax.ShapeDtypeStruct((cols + 16, width), jnp.int16), "hbm")],
                (0,),
                [
                    pltpu.VMEM((3 * tokens, width), bf16),
                    pltpu.VMEM((cols + 16, width), jnp.int16),
                    pltpu.VMEM((cols, 3 * tokens), bf16),
                    dma((3, count)),
                    dma((count,)),
                ],
                {},
                2 * cols * 3 * tokens * width,
                2 * width * (3 * tokens + cols),
                [other_grads, activations, two, three],
            )
            part = lax.ppermute(coded, "tensor", back)
            args += [activations, one, two, three, part]
        else:
            args += [gathered]
        aliases = {}
        for place, buffer in enumerate((new_momentum, record)):
            if buffer is not None:
                aliases[len(args)] = place
                args.append(buffer)
        return call(
            functools.partial(grad_kernel, n_act, line, slots, count, start, base),
            [
                (jax.ShapeDtypeStruct(momentum.shape, f32), "hbm"),
                (jax.ShapeDtypeStruct((n_rows, group_width), f32), "hbm"),
            ],
            (0, 1),
            [
                pltpu.VMEM((count, SUB, cols), f32),
                pltpu.VMEM((count, spans, slots, SUB), jnp.int32),
                pltpu.VMEM((count, n_tensor * tokens, SUB), bf16),
                pltpu.VMEM((count, cols + 16, SUB), jnp.int16),
                pltpu.VMEM((count, SUB, cols), f32),
                pltpu.VMEM((count, n_rows, SUB), f32),
                pltpu.VMEM((cols, SUB), f32),
                pltpu.VMEM((cols, SUB), f32),
                pltpu.VMEM((cols, SUB), f32),
                pltpu.VMEM((cols, SUB), f32),
                pltpu.VMEM((cols, n_tensor * tokens), bf16),
                dma((n_act + 3, count)),
                dma((2, count)),
            ],
            aliases,
            2 * cols * n_tensor * tokens * width + 12 * cols * cols * width,
            width * (8 * cols + 10 * tokens),
            args,
        )

    counts = [edges[group[-1] + 1] - edges[group[0]] for group in GROUPS]
    split = 2 if n_dp % 2 == 0 and all(n % 2 == 0 for n in counts) else 1
    new_momentum, decoded, square_list = None, None, []
    for group in GROUPS:
        base, count = edges[group[0]] * SUB, edges[group[-1] + 1] - edges[group[0]]
        width = count * SUB
        record = None
        for c in group:
            new_momentum, record = add_chunk(c, base, width, new_momentum, record)
        near = [record]
        for k in range(1, n_dp // 2):
            near.append(lax.ppermute(record, "dp", [(i, i ^ (2 * k)) for i in range(n_dp)]))
        args = [basis]
        for r in near:
            args += [r, lax.ppermute(r, "dp", [(i, i ^ 1) for i in range(n_dp)])]
        aliases = {}
        if decoded is not None:
            aliases = {len(args): 0}
            args.append(decoded)
        decoded, squares = call(
            functools.partial(sum_kernel, n_dp, slots, count // split, base // split, split),
            [
                (jax.ShapeDtypeStruct((cols, rows // split), f32), "hbm"),
                (jax.ShapeDtypeStruct((1, width // split), f32), "vmem"),
            ],
            (0,),
            [
                pltpu.VMEM((n_dp, count // split, n_rows, SUB), f32),
                pltpu.VMEM((count // split, cols, SUB), f32),
                pltpu.VMEM((2, n_dp, slots, spans, SUB), jnp.int32),
                pltpu.VMEM((cols, SUB), f32),
                pltpu.VMEM((cols, SUB), f32),
                dma((n_dp, count // split)),
                dma((count // split,)),
            ],
            aliases,
            6 * cols * cols * width,
            width * 4 * (cols + n_dp * n_rows),
            args,
        )
        square_list.append(squares)
    squares = jnp.concatenate(square_list, axis=1)
    if line:
        sq_args = [squares]
        for k in range(n_tensor - 1, 0, -1):
            pairs = [(i, i ^ k) for i in range(n_tensor)]
            sq_args.append(lax.ppermute(squares, "tensor", pairs))
    else:
        sq_args = [lax.psum(squares, "tensor")]
    n_mine = n_tiles // split
    update, half = call(
        functools.partial(scale_kernel, len(sq_args), cols * n_tensor, n_mine, split),
        [
            (jax.ShapeDtypeStruct((rows, cols), bf16), "hbm"),
            (jax.ShapeDtypeStruct((n_mine, SUB, cols), bf16), "vmem"),
        ],
        range(1, 1 + len(sq_args)),
        [pltpu.VMEM((n_mine, cols, SUB), f32), dma((n_mine,)), dma((n_mine,))],
        {},
        rows * cols,
        rows * cols * 6,
        [decoded] + sq_args,
    )
    if split == 2:
        half = lax.ppermute(half, "dp", [(i, i ^ 1) for i in range(n_dp)])
        (update,) = call(
            functools.partial(place_kernel, n_mine, split),
            [(jax.ShapeDtypeStruct((rows, cols), bf16), "hbm")],
            (0,),
            [dma((n_mine,))],
            {1: 0},
            rows * cols,
            rows * cols * 2,
            [half, update],
        )
    return new_momentum, update


def solution(mesh):
    placed = (
        P("dp", None, "tensor"),
        P(("dp", "tensor"), None),
        P("dp", "tensor"),
        P("dp", "tensor", None, None),
    )
    return jax.shard_map(
        body,
        mesh=mesh,
        in_specs=placed,
        out_specs=(P("dp", None, "tensor"), P(None, "tensor")),
        check_vma=False,
    )
```

```python
import functools

import jax
import jax.numpy as jnp
import numpy as np
from jax import lax
from jax.experimental import pallas as pl
from jax.experimental.pallas import tpu as pltpu
from jax.sharding import PartitionSpec as P


SPAN = 64
SUB = 256
LANES = 128
SUBLANES = 8
CODE_TOP = 32764.0
LN2 = 0.6931471805599453
VMEM_LIMIT = 16 * 1024 * 1024
CHUNKS = (4, 4, 6, 6)
GROUPS = ((0, 1), (2,), (3,))


def basis_parts():
    freq = np.arange(SPAN, dtype=np.float64)[:, None]
    place = np.arange(SPAN, dtype=np.float64)[None, :]
    scales = np.where(freq == 0, (1.0 / SPAN) ** 0.5, (2.0 / SPAN) ** 0.5)
    table = scales * np.cos(np.pi * (2.0 * place + 1.0) * freq / (2 * SPAN))
    table = table.astype(np.float32)
    high = table.astype(jnp.bfloat16)
    low = (table - high.astype(np.float32)).astype(jnp.bfloat16)
    return np.stack([np.concatenate(p, axis=1) for p in ((high, high, low), (high.T, high.T, low.T))])


def dot32(a, b):
    return lax.dot_general(a, b, (((1,), (0,)), ((), ())), preferred_element_type=jnp.float32)


def dot_split(triple, x):
    high = x.astype(jnp.bfloat16)
    low = (x - high.astype(jnp.float32)).astype(jnp.bfloat16)
    outs = []
    for at in range(0, x.shape[0], SPAN):
        part = high[at : at + SPAN]
        outs.append(dot32(triple, jnp.concatenate([part, low[at : at + SPAN], part], axis=0)))
    return jnp.concatenate(outs, axis=0)


def lanes_at(i, offset=0):
    return pl.ds(pl.multiple_of(offset + i * SUB, SUB), SUB)


def line_blocks(grads_ref, tokens, roles):
    index = lax.axis_index("tensor")
    middle = (index == 1) | (index == 2)
    sources = (index, 3 * (index - 1), 3 - index, 6 - 3 * index)
    parts = []
    for k in roles:
        at = pl.multiple_of(jnp.clip(sources[k], 0, 3) * tokens, tokens)
        part = grads_ref[pl.ds(at, tokens)].T
        parts.append(part if k == 0 else jnp.where(middle, part, jnp.zeros_like(part)))
    return jnp.concatenate(parts, axis=1)


def pairs_of(count, work):
    lax.fori_loop(0, count // 2, lambda i, c: work((2 * i, 2 * i + 1)), None)
    if count % 2:
        work((count - 1,))


def partial_kernel(count, start, grads_ref, *refs):
    act_refs, out_ref, blocks_ref = refs[:3], refs[3], refs[4]
    cols, tokens = grads_ref.shape[1], act_refs[1].shape[0]
    blocks_ref[...] = line_blocks(grads_ref, tokens, (0, 2, 3))

    def one(i):
        acts = [r[:, lanes_at(i, 0 if k else start)] for k, r in enumerate(act_refs)]
        part = dot32(blocks_ref[...], jnp.concatenate(acts, axis=0))
        top = jnp.maximum(jnp.max(jnp.abs(part), axis=0, keepdims=True), 1e-30)
        level = jnp.floor(jnp.log(top) * (1.0 / LN2)) + 1.0
        code = jnp.round(part * (CODE_TOP * jnp.exp(-level * LN2)))
        out_ref[:cols, lanes_at(i)] = code.astype(jnp.int32).astype(jnp.int16)
        extra = jnp.broadcast_to(level.astype(jnp.int32), (out_ref.shape[0] - cols, SUB))
        out_ref[cols:, lanes_at(i)] = extra.astype(jnp.int16)

    def work(tiles):
        for i in tiles:
            one(i)

    pairs_of(count, work)


def grad_kernel(n_act, has_part, slots, count, start, base, *refs):
    basis_ref, grads_ref, moment_ref, picks_ref = refs[:4]
    act_refs = refs[4 : 4 + n_act]
    part_ref = refs[4 + n_act] if has_part else None
    new_ref, record_ref, new_buf = refs[-9:-6]
    coeffs_refs, tile_refs, blocks_ref, out_sem = refs[-6:-4], refs[-4:-2], *refs[-2:]
    cols = moment_ref.shape[2]
    spans = cols // SPAN
    tokens = act_refs[0].shape[0]
    ids = lax.broadcasted_iota(jnp.int32, (SUBLANES, LANES), 0)

    def copy_out(i):
        return pltpu.make_async_copy(
            new_buf.at[i], new_ref.at[0, lanes_at(i, start)], out_sem.at[i]
        )

    if n_act > 1:
        blocks_ref[...] = line_blocks(grads_ref, tokens, (0, 1, 2, 3))
    else:
        blocks_ref[...] = grads_ref[...].T

    def gather(i, coeffs_ref):
        acts = [r[:, lanes_at(i, 0 if k else start)] for k, r in enumerate(act_refs)]
        acts = jnp.concatenate(acts, axis=0) if n_act > 1 else acts[0]
        total = 0.9 * moment_ref[0, lanes_at(i, start)].T + dot32(blocks_ref[...], acts)
        if has_part:
            level = part_ref[cols:, lanes_at(i)][:1].astype(jnp.int32).astype(jnp.float32)
            code = part_ref[:cols, lanes_at(i)].astype(jnp.int32).astype(jnp.float32)
            total = total + code * (jnp.exp(level * LN2) * (1.0 / CODE_TOP))
        coeffs_ref[...] = dot_split(basis_ref[0], total)
        return total

    def pick(i, coeffs_ref, tile_ref):
        for lo in range(0, SUB, LANES):
            lanes = slice(lo, lo + LANES)
            read = pl.ds(pl.multiple_of(start + i * SUB + lo, LANES), LANES)
            write = pl.ds(pl.multiple_of(start - base + i * SUB + lo, LANES), LANES)
            for b in range(spans):
                rows = [b * SPAN + h * SUBLANES for h in range(SPAN // SUBLANES)]
                blocks = [coeffs_ref[at : at + SUBLANES, lanes] for at in rows]
                parts = [jnp.zeros((SUBLANES, LANES), jnp.float32)] * len(rows)
                code = jnp.zeros((1, LANES), jnp.int32)
                for j in range(slots):
                    place = picks_ref[0, b, j : j + 1, read]
                    offset = place - ids
                    value = jnp.zeros((SUBLANES, LANES), jnp.float32)
                    for h in range(len(rows)):
                        hit = offset == h * SUBLANES
                        value = jnp.where(hit, blocks[h], value)
                        parts[h] = jnp.where(hit, blocks[h], parts[h])
                    value = jnp.sum(value, axis=0, keepdims=True)
                    record_ref[b * slots + j : b * slots + j + 1, write] = value
                    code = code + place * SPAN**j
                for at, part in zip(rows, parts):
                    tile_ref[at : at + SUBLANES, lanes] = part
                row = spans * slots + b
                record_ref[row : row + 1, write] = code.astype(jnp.float32)

    def finish(i, total, tile_ref):
        restored = dot_split(basis_ref[1], tile_ref[...])
        new_buf[i] = (total - restored).T
        copy_out(i).start()

    def work(tiles):
        totals = [gather(i, coeffs_refs[k]) for k, i in enumerate(tiles)]
        for k, i in enumerate(tiles):
            pick(i, coeffs_refs[k], tile_refs[k])
            finish(i, totals[k], tile_refs[k])

    pairs_of(count, work)
    for i in range(count):
        copy_out(i).wait()


def tile_of(i, split, ahead=0):
    return i * split + (lax.axis_index("dp") + ahead) % split


def sum_kernel(n_rec, slots, count, base, split, *refs):
    basis_ref = refs[0]
    record_refs = refs[1 : 1 + n_rec]
    decoded_ref, squares_ref, place_ref = refs[-5:-2]
    tile_refs = refs[-2:]
    cols = decoded_ref.shape[0]
    spans = cols // SPAN
    ids = lax.broadcasted_iota(jnp.int32, (SUBLANES, LANES), 0)

    def spread(slot, i):
        tile_at = tile_of(i, split)
        for k in range(n_rec):
            code = record_refs[k][spans * slots :, lanes_at(tile_at)].astype(jnp.int32)
            for j in range(slots):
                place_ref[slot, k, j] = lax.shift_right_logical(code, 6 * j) & (SPAN - 1)
        for lo in range(0, SUB, LANES):
            lanes = slice(lo, lo + LANES)
            read = pl.ds(pl.multiple_of(tile_at * SUB + lo, LANES), LANES)
            for b in range(spans):
                stack = []
                for k in range(n_rec):
                    parts = [jnp.zeros((SUBLANES, LANES), jnp.float32)] * (SPAN // SUBLANES)
                    for j in range(slots):
                        place = place_ref[slot, k, j, b : b + 1, lanes] - ids
                        value = record_refs[k][b * slots + j : b * slots + j + 1, read]
                        value = jnp.broadcast_to(value, (SUBLANES, LANES))
                        for h in range(SPAN // SUBLANES):
                            parts[h] = jnp.where(place == h * SUBLANES, value, parts[h])
                    stack.append(parts)
                    done = k + 1
                    while done % 2 == 0:
                        right = stack.pop()
                        stack[-1] = [x + y for x, y in zip(stack[-1], right)]
                        done //= 2
                for h, part in enumerate(stack[0]):
                    at = b * SPAN + h * SUBLANES
                    tile_refs[slot][at : at + SUBLANES, lanes] = part

    def decode(slot, i):
        decoded = dot_split(basis_ref[1], tile_refs[slot][...])
        decoded_ref[:, lanes_at(i, base)] = decoded
        squares_ref[:, lanes_at(i)] = jnp.sum(decoded * decoded, axis=0, keepdims=True)

    def work(tiles):
        for slot, i in enumerate(tiles):
            spread(slot, i)
            decode(slot, i)

    pairs_of(count, work)


def scale_kernel(n_sq, n_all, count, split, *refs):
    decoded_ref, sq_refs = refs[0], refs[1 : 1 + n_sq]
    out_ref, half_ref, out_sem = refs[-3:]

    def copy_out(i):
        return pltpu.make_async_copy(
            half_ref.at[i], out_ref.at[lanes_at(tile_of(i, split))], out_sem.at[i]
        )

    def step(i, carry):
        total = sq_refs[0][:, lanes_at(i)]
        for ref in sq_refs[1:]:
            total = total + ref[:, lanes_at(i)]
        scale = 1.0 / jnp.sqrt(total * (1.0 / n_all) + 1e-05)
        half_ref[i] = (decoded_ref[:, lanes_at(i)] * scale).astype(jnp.bfloat16).T
        copy_out(i).start()
        return carry

    lax.fori_loop(0, count, step, 0)
    for i in range(count):
        copy_out(i).wait()


def place_kernel(count, split, half_ref, update_ref, out_ref, out_sem):
    def copy_out(i):
        return pltpu.make_async_copy(
            half_ref.at[i], out_ref.at[lanes_at(tile_of(i, split, 1))], out_sem.at[i]
        )

    for i in range(count):
        copy_out(i).start()
    for i in range(count):
        copy_out(i).wait()


def call(kernel, out_shape, in_hbm, scratch, aliases, flops, moved, args):
    vmem = pl.BlockSpec(memory_space=pltpu.VMEM)
    anywhere = pl.BlockSpec(memory_space=pl.ANY)
    many = [anywhere if where == "hbm" else vmem for _, where in out_shape]
    return pl.pallas_call(
        kernel,
        in_specs=[anywhere if k in in_hbm else vmem for k in range(len(args))],
        out_specs=many,
        out_shape=[shape for shape, _ in out_shape],
        scratch_shapes=scratch,
        input_output_aliases=aliases,
        compiler_params=pltpu.CompilerParams(vmem_limit_bytes=VMEM_LIMIT),
        cost_estimate=pl.CostEstimate(flops=flops, bytes_accessed=moved, transcendentals=0),
    )(*args)


def body(momentum, activations, out_grads, positions):
    rows, cols = momentum.shape[1:]
    spans, slots = positions.shape[1:3]
    tokens = activations.shape[0]
    n_tensor, n_dp = lax.axis_size("tensor"), lax.axis_size("dp")
    n_tiles = rows // SUB
    edges = [0]
    for c in CHUNKS:
        edges.append(edges[-1] + c)
    edges = [e * n_tiles // edges[-1] for e in edges]
    basis = jnp.asarray(basis_parts())
    n_rows = spans * slots + spans
    dma = pltpu.SemaphoreType.DMA
    f32, bf16 = jnp.float32, jnp.bfloat16

    line = n_tensor == 4
    if line:
        outer, back = [(0, 1), (3, 2)], [(1, 0), (2, 3)]
        inner = []
        for d in range(n_dp):
            for t, to in ((0, (d ^ 1, 0)), (1, (d, 2)), (2, (d, 1)), (3, (d ^ 1, 3))):
                inner.append((d * n_tensor + t, to[0] * n_tensor + to[1]))
        other_grads = lax.ppermute(out_grads, "tensor", outer)
        owns = []
        for c in range(len(CHUNKS)):
            owns.append(lax.slice_in_dim(activations, edges[c] * SUB, edges[c + 1] * SUB, axis=1))
    else:
        gathered = lax.all_gather(activations, "tensor", axis=0, tiled=True)

    def add_chunk(c, base, group_width, new_momentum, record):
        start, count = edges[c] * SUB, edges[c + 1] - edges[c]
        width = count * SUB
        args = [basis, out_grads, momentum, positions]
        n_act = 4 if line else 1
        if line:
            own = owns[c]
            one = lax.ppermute(own, "tensor", outer)
            two = lax.ppermute(own, ("dp", "tensor"), inner)
            three = lax.ppermute(one, ("dp", "tensor"), inner)
            (coded,) = call(
                functools.partial(partial_kernel, count, start),
                [(jax.ShapeDtypeStruct((cols + 8, width), jnp.int16), "vmem")],
                (),
                [pltpu.VMEM((cols, 3 * tokens), bf16)],
                {},
                2 * cols * 3 * tokens * width,
                2 * width * (3 * tokens + cols),
                [other_grads, activations, two, three],
            )
            part = lax.ppermute(coded, "tensor", back)
            args += [activations, one, two, three, part]
        else:
            args += [gathered]
        aliases, in_hbm = {}, ()
        for place, buffer in enumerate((new_momentum, record)):
            if buffer is not None:
                aliases[len(args)] = place
                in_hbm += (len(args),) if place == 0 else ()
                args.append(buffer)
        return call(
            functools.partial(grad_kernel, n_act, line, slots, count, start, base),
            [
                (jax.ShapeDtypeStruct(momentum.shape, f32), "hbm"),
                (jax.ShapeDtypeStruct((n_rows, group_width), f32), "vmem"),
            ],
            in_hbm,
            [
                pltpu.VMEM((count, SUB, cols), f32),
                pltpu.VMEM((cols, SUB), f32),
                pltpu.VMEM((cols, SUB), f32),
                pltpu.VMEM((cols, SUB), f32),
                pltpu.VMEM((cols, SUB), f32),
                pltpu.VMEM((cols, n_tensor * tokens), bf16),
                dma((count,)),
            ],
            aliases,
            2 * cols * n_tensor * tokens * width + 12 * cols * cols * width,
            width * (8 * cols + 10 * tokens),
            args,
        )

    counts = [edges[group[-1] + 1] - edges[group[0]] for group in GROUPS]
    split = 2 if n_dp % 2 == 0 and all(n % 2 == 0 for n in counts) else 1
    new_momentum, decoded, square_list = None, None, []
    for group in GROUPS:
        base, count = edges[group[0]] * SUB, edges[group[-1] + 1] - edges[group[0]]
        width = count * SUB
        record = None
        for c in group:
            new_momentum, record = add_chunk(c, base, width, new_momentum, record)
        near = [record]
        for k in range(1, n_dp // 2):
            near.append(lax.ppermute(record, "dp", [(i, i ^ (2 * k)) for i in range(n_dp)]))
        args = [basis]
        for r in near:
            args += [r, lax.ppermute(r, "dp", [(i, i ^ 1) for i in range(n_dp)])]
        aliases = {}
        if decoded is not None:
            aliases = {len(args): 0}
            args.append(decoded)
        decoded, squares = call(
            functools.partial(sum_kernel, n_dp, slots, count // split, base // split, split),
            [
                (jax.ShapeDtypeStruct((cols, rows // split), f32), "vmem"),
                (jax.ShapeDtypeStruct((1, width // split), f32), "vmem"),
            ],
            (),
            [
                pltpu.VMEM((2, n_dp, slots, spans, SUB), jnp.int32),
                pltpu.VMEM((cols, SUB), f32),
                pltpu.VMEM((cols, SUB), f32),
            ],
            aliases,
            6 * cols * cols * width,
            width * 4 * (cols + n_dp * n_rows),
            args,
        )
        square_list.append(squares)
    squares = jnp.concatenate(square_list, axis=1)
    if line:
        sq_args = [squares]
        for k in range(n_tensor - 1, 0, -1):
            pairs = [(i, i ^ k) for i in range(n_tensor)]
            sq_args.append(lax.ppermute(squares, "tensor", pairs))
    else:
        sq_args = [lax.psum(squares, "tensor")]
    n_mine = n_tiles // split
    update, half = call(
        functools.partial(scale_kernel, len(sq_args), cols * n_tensor, n_mine, split),
        [
            (jax.ShapeDtypeStruct((rows, cols), bf16), "hbm"),
            (jax.ShapeDtypeStruct((n_mine, SUB, cols), bf16), "vmem"),
        ],
        (),
        [dma((n_mine,))],
        {},
        rows * cols,
        rows * cols * 6,
        [decoded] + sq_args,
    )
    if split == 2:
        half = lax.ppermute(half, "dp", [(i, i ^ 1) for i in range(n_dp)])
        (update,) = call(
            functools.partial(place_kernel, n_mine, split),
            [(jax.ShapeDtypeStruct((rows, cols), bf16), "hbm")],
            (1,),
            [dma((n_mine,))],
            {1: 0},
            rows * cols,
            rows * cols * 2,
            [half, update],
        )
    return new_momentum, update


def solution(mesh):
    placed = (
        P("dp", None, "tensor"),
        P(("dp", "tensor"), None),
        P("dp", "tensor"),
        P("dp", "tensor", None, None),
    )
    return jax.shard_map(
        body,
        mesh=mesh,
        in_specs=placed,
        out_specs=(P("dp", None, "tensor"), P(None, "tensor")),
        check_vma=False,
    )
```
